128 devices in a mesh: row: 16 (over y_hi, x, core), orb: 8 (over y_lo, z).
Axes of the slice: x: 4, y: 4 (y_hi: 2, y_lo: 2; y = y_hi * 2 + y_lo), z: 4, core: 2. Of those that a mesh axis runs over, the one named last changes fastest.
Arguments:
- chol_vectors: bfloat16 [4, 8192, 8192], P(None, 'row', 'orb'), may hold values from -6 to 6
- orbitals: bfloat16 [8192, 1024], P('orb'), may hold values from -0.0078125 to 0.0078125
Outputs:
- exchange: float32 [8192, 8192], P(('row', 'orb'))
The draws below stay inside these ranges and needn't reach their ends.
All inputs are finite; a program needn't handle non-finite values.
Results may differ from the reference program's by a relative error of at most 0.0032.
Values may be sent and summed in bfloat16 or wider, within the bound.
No kernel may reach another device: no remote copies, remote signals or barrier semaphores. Data moves between devices by JAX's collectives and lax.ppermute only.
A program may use at most 128 MiB of HBM per device.

```python
import jax
import jax.numpy as jnp
from jax import lax

NB = 8192
NO = 1024
NCHOL = 4


def shard_levels(key, dims, pieces, least, top_value):
    def one(axis_at, parts):
        heights = jax.random.uniform(jax.random.fold_in(jax.random.fold_in(key, 6), axis_at), (parts,), jnp.float32, least / len(pieces), top_value / len(pieces))
        return jnp.repeat(jnp.exp(heights), dims[axis_at] // parts).reshape((-1,) + (1,) * (len(dims) - axis_at - 1))

    gain = one(*pieces[0])
    for cut in pieces[1:]:
        gain = gain * one(*cut)
    return gain


def gaussian(own_key, extent, width, limit, shards=(), kind=jnp.bfloat16):
    loudness = shard_levels(own_key, extent, shards, -0.22, 0.18) if shards else 1.0
    drawn = jax.random.normal(own_key, extent, jnp.float32) * width * loudness
    return jnp.minimum(jnp.maximum(drawn, -limit), limit).astype(kind)


def setup_inputs(seed: int = 0) -> dict:
    key_list = jax.random.split(jax.random.key(seed), 3)
    return {
        "chol_vectors": gaussian(key_list[0], (NCHOL, NB, NB), 1.0, 6.0, ((1, 16), (2, 8))),
        "orbitals": gaussian(key_list[1], (NB, NO), (NB * 64) ** -0.5, 0.0078125, ((0, 8),)),
    }


def reference(chol_vectors, orbitals):
    coeffs = orbitals.astype(jnp.float32)
    exchange = jnp.zeros((NB, NB), jnp.float32)
    for vector in range(NCHOL):
        half_vec = jnp.dot(chol_vectors[vector].astype(jnp.float32), coeffs, precision=lax.Precision.HIGHEST)
        half_vec = half_vec.astype(jnp.bfloat16).astype(jnp.float32)
        exchange = exchange + jnp.dot(half_vec, half_vec.T, precision=lax.Precision.HIGHEST)
    return exchange
```

```python
import functools

import jax
import jax.numpy as jnp
from jax import lax
from jax.experimental import pallas as pl
from jax.experimental.pallas import tpu as pltpu
from jax.sharding import PartitionSpec as P

AXES = ("row", "orb")
NX, NY, NZ, NC = 4, 4, 4, 2
F16_TOP = 32768.0
OTHERS = ((1, 2), (0, 2), (1, 1), (0, 1), (1, 3), (0, 3), (1, 0))
MEMBERS = ((0, 0),) + OTHERS
FIRST = ((0, 0), (1, 0), (0, 1), (0, 3))
SECOND = ((1, 1), (1, 3), (0, 2), (1, 2))
PANELS = FIRST + SECOND


def device_at(x, y, z, c):
    x, y, z, c = x % NX, y % NY, z % NZ, c % NC
    row = ((y // 2) * NX + x) * NC + c
    return row * 8 + (y % 2) * NZ + z


def send(value, target):
    pairs = [
        (device_at(x, y, z, c), device_at(*target(x, y, z, c)))
        for x in range(NX)
        for y in range(NY)
        for z in range(NZ)
        for c in range(NC)
    ]
    return lax.ppermute(value, AXES, pairs)


def to_orb(dy, k):
    return lambda x, y, z, c: (x, y ^ dy, z + k, c)


def to_x(k):
    return lambda x, y, z, c: (x + k, y, z, c)


def to_half(x, y, z, c):
    return x, y ^ 2, z, c


def to_core(x, y, z, c):
    return x, y, z, c ^ 1


def same_rows(x, y, z, c):
    return x, y ^ c, z, c


def other_rows(x, y, z, c):
    return (x, y, z, 0) if c else (x, y ^ 1, z, 1)


def to_panel(k):
    return lambda x, y, z, c: (x, (y & 2) | c, z + k, (y & 1) ^ c)


def product_kernel(pieces, *refs):
    left, right, outs = refs[: 2 * NZ], refs[2 * NZ : 2 * NZ + pieces], refs[2 * NZ + pieces :]
    vectors, width = left[0].shape[0], right[0].shape[2]
    for pair in range(0, pieces, 2):
        for j in range(2):
            value = None
            for k in range(NZ):
                for p in range(0, vectors, 2):
                    l = jnp.concatenate([left[j * NZ + k][p], left[j * NZ + k][p + 1]], axis=1)
                    r = jnp.concatenate(
                        [
                            jnp.concatenate([right[q][k, p], right[q][k, p + 1]], axis=1)
                            for q in (pair, pair + 1)
                        ],
                        axis=0,
                    )
                    term = lax.dot_general(
                        l, r, (((1,), (1,)), ((), ())), preferred_element_type=jnp.float32
                    )
                    value = term if value is None else value + term
            outs[j][:, pair * width : (pair + 2) * width] = value


def product(left, right):
    pieces = len(right)
    vectors, rows, depth = left[0].shape
    columns = right[0].shape[2] * pieces
    whole = pl.BlockSpec(memory_space=pltpu.VMEM)
    return pl.pallas_call(
        functools.partial(product_kernel, pieces),
        in_specs=[whole] * (2 * NZ + pieces),
        out_specs=[whole] * 2,
        out_shape=[jax.ShapeDtypeStruct((rows, columns), jnp.float32)] * 2,
        compiler_params=pltpu.CompilerParams(vmem_limit_bytes=40 << 20),
        cost_estimate=pl.CostEstimate(
            flops=4 * rows * columns * depth * vectors * NZ,
            bytes_accessed=12 << 20,
            transcendentals=0,
        ),
        name="product",
    )(*left, *right)


def split_kernel(where, *refs):
    own, got, outs = refs[:2], refs[2:4], refs[4:]
    y, z = where[0], where[1]
    columns = own[0].shape[1]
    for (dy, k), out in zip(MEMBERS, outs):
        start = (lax.rem(y + dy, 2) * NZ + lax.rem(z + k, NZ)) * 64
        rows = pl.ds(pl.multiple_of(start, 64), 64)
        for h in range(2):
            total = own[h][rows, :] + got[h][rows, :]
            out[:, h * columns : (h + 1) * columns] = total.astype(out.dtype)


def split(where, own, got):
    columns = own[0].shape[1] * 2
    whole = pl.BlockSpec(memory_space=pltpu.VMEM)
    return pl.pallas_call(
        split_kernel,
        grid_spec=pltpu.PrefetchScalarGridSpec(
            num_scalar_prefetch=1, grid=(), in_specs=[whole] * 4, out_specs=[whole] * 8
        ),
        out_shape=[
            jax.ShapeDtypeStruct((64, columns), jnp.bfloat16 if i else jnp.float32)
            for i in range(8)
        ],
        cost_estimate=pl.CostEstimate(flops=1 << 20, bytes_accessed=5 << 20, transcendentals=0),
        name="split",
    )(where, *own, *got)


def place_kernel(where, *refs):
    ins, out = refs[:-1], refs[-1]
    y, z, x, half = where[0], where[1], where[2], where[3]
    for (dy, k), ref in zip(MEMBERS, ins):
        member = lax.rem(y + dy, 2) * NZ + lax.rem(z + NZ - k, NZ)
        for n, (dh, kx) in enumerate(PANELS):
            block = lax.rem(half + dh, 2) * NX + lax.rem(x + NX - kx, NX)
            start = pl.multiple_of(block * 1024 + member * 128, 128)
            out[:, pl.ds(start, 128)] = ref[:, n * 128 : (n + 1) * 128].astype(out.dtype)


def place(where, parts):
    whole = pl.BlockSpec(memory_space=pltpu.VMEM)
    rows, columns = parts[0].shape
    return pl.pallas_call(
        place_kernel,
        grid_spec=pltpu.PrefetchScalarGridSpec(
            num_scalar_prefetch=1, grid=(), in_specs=[whole] * 8, out_specs=whole
        ),
        out_shape=jax.ShapeDtypeStruct((rows, columns * 8), jnp.float32),
        cost_estimate=pl.CostEstimate(flops=1 << 20, bytes_accessed=3 << 20, transcendentals=0),
        name="place",
    )(where, *parts)


def on_device(chol_vectors, orbitals):
    vectors, rows, contracted = chol_vectors.shape
    width = orbitals.shape[1] // 8
    row, orb = lax.axis_index("row"), lax.axis_index("orb")
    z, y = orb % NZ, orb // NZ
    x, half = (row // NC) % NX, row // (NC * NX)
    where = jnp.stack([y, z, x, half]).astype(jnp.int32)

    bound = (
        jnp.max(jnp.abs(orbitals)).astype(jnp.float32)
        * jnp.max(jnp.abs(chol_vectors)).astype(jnp.float32)
        * contracted
    )
    bound = jnp.maximum(bound, 1e-30)
    scale = F16_TOP / bound

    def term(dy, k):
        start = (((y + dy) % 2) * NZ + (z + k) % NZ) * width
        block = lax.dynamic_slice_in_dim(orbitals, start, width, axis=1)
        return jnp.einsum("prm,mi->pri", chol_vectors, block, preferred_element_type=jnp.float32)

    got = [send((term(dy, k) * scale).astype(jnp.float16), to_orb(dy, k)) for dy, k in OTHERS]
    tile = jnp.full((8, 128), bound)
    bounds_y = (tile, send(tile, to_orb(1, 0)))
    bounds = {(dy, 0): bounds_y[dy][0, 0] for dy in range(2)}
    both = jnp.concatenate(bounds_y, axis=0)
    for k in range(1, NZ):
        there = send(both, to_orb(0, k))
        bounds[0, k], bounds[1, k] = there[0, 0], there[8, 0]
    total = term(0, 0)
    for member, value in zip(OTHERS, got):
        total = total + value.astype(jnp.float32) * (bounds[member] * (1.0 / F16_TOP))
    half_vec = total.astype(jnp.bfloat16)

    a0 = send(half_vec, same_rows)
    a1 = send(half_vec, other_rows)
    panel = jnp.stack(
        [
            send(
                lax.dynamic_slice_in_dim(half_vec, ((z + k) % NZ) * 128, 128, axis=1), to_panel(k)
            )
            for k in range(NZ)
        ]
    )
    left = {(0, 0): a0, (1, 0): a1}
    left[0, 1] = send(a0, to_orb(0, 1))
    left[1, 3] = send(a1, to_orb(0, 3))
    left[1, 1] = send(a1, to_orb(0, 1))
    left[0, 3] = send(a0, to_orb(0, 3))
    left[0, 2] = send(left[0, 1], to_orb(0, 1))
    left[1, 2] = send(left[1, 3], to_orb(0, 3))
    right = {(0, 0): panel}
    right[1, 0] = send(panel, to_half)
    right[0, 1] = send(panel, to_x(1))
    right[0, 3] = send(panel, to_x(3))
    right[1, 1] = send(right[1, 0], to_x(1))
    right[1, 3] = send(right[1, 0], to_x(3))
    right[0, 2] = send(right[0, 1], to_x(1))
    right[1, 2] = send(right[1, 3], to_x(3))
    lefts = [left[j, k] for j in range(2) for k in range(NZ)]
    own, got = [], []
    for names in (FIRST, SECOND):
        mine, others = product(lefts, [right[n] for n in names])
        own.append(mine)
        got.append(send(others, to_core))
    parts = split(where, own, got)
    parts = [parts[0]] + [send(v, to_orb(dy, k)) for (dy, k), v in zip(OTHERS, parts[1:])]
    return place(where, parts)


def solution(mesh):
    return jax.shard_map(
        on_device,
        mesh=mesh,
        in_specs=(P(None, "row", "orb"), P("orb", None)),
        out_specs=P(("row", "orb"), None),
        check_vma=False,
    )
```

```python
import functools

import jax
import jax.numpy as jnp
from jax import lax
from jax.experimental import pallas as pl
from jax.experimental.pallas import tpu as pltpu
from jax.sharding import PartitionSpec as P


AXES = ("row", "orb")
NX, NY, NZ, NC = 4, 4, 4, 2
F16_TOP = 32768.0
OTHERS = ((1, 2), (0, 2), (1, 1), (0, 1), (1, 3), (0, 3), (1, 0))
MEMBERS = ((0, 0),) + OTHERS
PANELS = ((0, 0), (1, 0), (0, 1), (0, 3), (1, 1), (1, 3), (0, 2), (1, 2))
EARLY = 6


def device_at(x, y, z, c):
    x, y, z, c = x % NX, y % NY, z % NZ, c % NC
    row = ((y // 2) * NX + x) * NC + c
    return row * 8 + (y % 2) * NZ + z


def send(value, target):
    pairs = [
        (device_at(x, y, z, c), device_at(*target(x, y, z, c)))
        for x in range(NX)
        for y in range(NY)
        for z in range(NZ)
        for c in range(NC)
    ]
    return lax.ppermute(value, AXES, pairs)


def to_orb(dy, k):
    return lambda x, y, z, c: (x, y ^ dy, z + k, c)


def to_x(k):
    return lambda x, y, z, c: (x + k, y, z, c)


def to_core(x, y, z, c):
    return x, y, z, c ^ 1


def to_panel(k):
    return lambda x, y, z, c: (x, (y & 2) | c, z + k, (y & 1) ^ c)


def to_half(x, y, z, c):
    return x, y ^ 2, z, c


def peak_of(block):
    return jnp.max(jnp.max(jnp.abs(block), axis=0, keepdims=True).astype(jnp.float32))


def pair_columns(where, k, c_ref):
    y, z = where[0], where[1]
    blocks = []
    for dy in range(2):
        start = (lax.rem(y + dy, 2) * NZ + lax.rem(z + k, NZ)) * 128
        blocks.append(c_ref[:, pl.ds(pl.multiple_of(start, 128), 128)])
    return jnp.concatenate(blocks, axis=1)


def first_kernel(k, where, l_ref, c_ref, out0, out1, bound, scale):
    terms_kernel(k, where, l_ref, c_ref, out0, out1)
    peak = peak_of(l_ref[0])
    for p in range(1, l_ref.shape[0]):
        peak = jnp.maximum(peak, peak_of(l_ref[p]))
    limit = jnp.maximum(peak * peak_of(c_ref[...]) * l_ref.shape[2], 1e-30)
    bound[...] = jnp.full(bound.shape, limit)
    scale[...] = jnp.full(bound.shape, F16_TOP / limit)


def first_terms(where, chol_vectors, orbitals, k):
    vectors, rows, contracted = chol_vectors.shape
    whole = pl.BlockSpec(memory_space=pltpu.VMEM)
    return pl.pallas_call(
        functools.partial(first_kernel, k),
        grid_spec=pltpu.PrefetchScalarGridSpec(
            num_scalar_prefetch=1, grid=(), in_specs=[whole] * 2, out_specs=[whole] * 4
        ),
        out_shape=[jax.ShapeDtypeStruct((vectors, rows, 128), jnp.float32)] * 2
        + [jax.ShapeDtypeStruct((8, 128), jnp.float32)] * 2,
        compiler_params=pltpu.CompilerParams(vmem_limit_bytes=20 << 20),
        cost_estimate=pl.CostEstimate(
            flops=2 * vectors * rows * contracted * 256, bytes_accessed=8 << 20, transcendentals=0
        ),
        name="first_terms",
    )(where, chol_vectors, orbitals)


def terms_kernel(k, where, l_ref, c_ref, out0, out1):
    columns = pair_columns(where, k, c_ref)
    for p in range(l_ref.shape[0]):
        terms = jnp.dot(l_ref[p], columns, preferred_element_type=jnp.float32)
        out0[p] = terms[:, :128]
        out1[p] = terms[:, 128:]


def more_terms(where, vecs, orbitals, k):
    vectors, rows, contracted = vecs.shape
    whole = pl.BlockSpec(memory_space=pltpu.VMEM)
    return pl.pallas_call(
        functools.partial(terms_kernel, k),
        grid_spec=pltpu.PrefetchScalarGridSpec(
            num_scalar_prefetch=1, grid=(), in_specs=[whole] * 2, out_specs=[whole] * 2
        ),
        out_shape=[jax.ShapeDtypeStruct((vectors, rows, 128), jnp.float32)] * 2,
        compiler_params=pltpu.CompilerParams(vmem_limit_bytes=20 << 20),
        cost_estimate=pl.CostEstimate(
            flops=2 * vectors * rows * contracted * 256, bytes_accessed=8 << 20, transcendentals=0
        ),
        name="more_terms",
    )(where, vecs, orbitals)


def product_kernel(parts, done, where, *refs):
    left, refs = refs[: 2 * NZ], refs[2 * NZ :]
    count = sum(parts)
    mine, others = [], []
    for pieces, flat in ((mine, refs[:count]), (others, refs[count : 2 * count])):
        for n in parts:
            pieces.append(flat[:n])
            flat = flat[n:]
    before, outs, total = refs[2 * count : -9], refs[-9:-1], refs[-1]
    y, z, c = where[0], where[1], where[4]
    vectors, width = left[0].shape[0], mine[0][0].shape[2]

    def tile(piece, k, v):
        per = NZ // len(piece)
        return piece[k // per][k % per, v]

    for ref, out in zip(before, outs):
        out[:, :done] = ref[...]
    for pair in range(0, len(parts), 2):
        value = None
        for dy in range(2):
            for k in range(NZ):
                for p in range(0, vectors, 2):
                    l = jnp.concatenate([left[dy * NZ + k][p], left[dy * NZ + k][p + 1]], axis=1)
                    blocks = []
                    for q in (pair, pair + 1):
                        row = [
                            jnp.where(c == dy, tile(mine[q], k, v), tile(others[q], k, v))
                            for v in (p, p + 1)
                        ]
                        blocks.append(jnp.concatenate(row, axis=1))
                    term = lax.dot_general(
                        l,
                        jnp.concatenate(blocks, axis=0),
                        (((1,), (1,)), ((), ())),
                        preferred_element_type=jnp.float32,
                    )
                    value = term if value is None else value + term
        total[...] = value
        for (dy, k), out in zip(MEMBERS, outs):
            start = (lax.rem(y + dy, 2) * NZ + lax.rem(z + k, NZ)) * 64
            rows = total[pl.ds(pl.multiple_of(start, 64), 64), :]
            at = done + pair * width
            out[:, at : at + 2 * width] = rows.astype(out.dtype)


def product(where, left, mine, others, before=()):
    parts = tuple(len(m) for m in mine)
    vectors, rows, depth = left[0].shape
    width = mine[0][0].shape[2]
    done = before[0].shape[1] if before else 0
    columns = done + len(parts) * width
    whole = pl.BlockSpec(memory_space=pltpu.VMEM)
    return pl.pallas_call(
        functools.partial(product_kernel, parts, done),
        grid_spec=pltpu.PrefetchScalarGridSpec(
            num_scalar_prefetch=1,
            grid=(),
            in_specs=[whole] * (2 * NZ + 2 * sum(parts) + len(before)),
            out_specs=[whole] * 8,
            scratch_shapes=[pltpu.VMEM((rows, 2 * width), jnp.float32)],
        ),
        out_shape=[
            jax.ShapeDtypeStruct((64, columns), jnp.bfloat16 if i else jnp.float32)
            for i in range(8)
        ],
        compiler_params=pltpu.CompilerParams(vmem_limit_bytes=40 << 20),
        cost_estimate=pl.CostEstimate(
            flops=4 * rows * len(parts) * width * depth * vectors * NZ,
            bytes_accessed=12 << 20,
            transcendentals=0,
        ),
        name="product",
    )(where, *left, *sum(mine, []), *sum(others, []), *before)


def place_kernel(where, *refs):
    ins, out = refs[:-1], refs[-1]
    y, z, x, half = where[0], where[1], where[2], where[3]
    for i, (dy, k) in enumerate(MEMBERS):
        member = lax.rem(y + dy, 2) * NZ + lax.rem(z + NZ - k, NZ)
        for n, (dh, kx) in enumerate(PANELS):
            block = lax.rem(half + dh, 2) * NX + lax.rem(x + NX - kx, NX)
            start = pl.multiple_of(block * 1024 + member * 128, 128)
            out[:, pl.ds(start, 128)] = ins[i][:, n * 128 : (n + 1) * 128].astype(out.dtype)


def place(where, parts):
    whole = pl.BlockSpec(memory_space=pltpu.VMEM)
    rows, columns = parts[0].shape
    return pl.pallas_call(
        place_kernel,
        grid_spec=pltpu.PrefetchScalarGridSpec(
            num_scalar_prefetch=1, grid=(), in_specs=[whole] * 8, out_specs=whole
        ),
        out_shape=jax.ShapeDtypeStruct((rows, columns * 8), jnp.float32),
        cost_estimate=pl.CostEstimate(flops=1 << 20, bytes_accessed=3 << 20, transcendentals=0),
        name="place",
    )(where, *parts)


def exchange(chol_vectors, orbitals):
    row, orb = lax.axis_index("row"), lax.axis_index("orb")
    z, y = orb % NZ, orb // NZ
    x, half, core = (row // NC) % NX, row // (NC * NX), row % NC
    where = jnp.stack([y, z, x, half, core]).astype(jnp.int32)

    terms = {}
    terms[0, 2], terms[1, 2], tile, scale = first_terms(where, chol_vectors, orbitals, 2)
    for k in (1, 3, 0):
        terms[0, k], terms[1, k] = more_terms(where, chol_vectors, orbitals, k)
    got = []
    for k in (2, 1, 3, 0):
        pair = (terms[0, k], terms[1, k], scale) if k else (terms[1, k], scale)
        *pair, by = lax.optimization_barrier(pair)
        pair = [(v * by[0]).astype(jnp.float16) for v in pair]
        got.append(send(pair[-1], to_orb(1, k)))
        if k:
            got.append(send(pair[0], to_orb(0, k)))
    bounds_y = (tile, send(tile, to_orb(1, 0)))
    bounds = {(1, 0): bounds_y[1][0]}
    both = jnp.concatenate(bounds_y, axis=0)
    for k in range(1, NZ):
        there = send(both, to_orb(0, k))
        bounds[0, k], bounds[1, k] = there[0], there[8]
    total = terms[0, 0]
    for i, (member, value) in enumerate(zip(OTHERS, got)):
        total = total + value.astype(jnp.float32) * (bounds[member] * (1.0 / F16_TOP))
        if i == 4:
            total = lax.optimization_barrier(total)
    half_vec = total.astype(jnp.bfloat16)

    left = {(0, 0): half_vec, (1, 0): send(half_vec, to_orb(1, 0))}
    slices = [
        lax.dynamic_slice_in_dim(half_vec, ((z + k) % NZ) * 128, 128, axis=1) for k in range(NZ)
    ]
    panel = jnp.stack([send(slices[k], to_panel(k)) for k in range(NZ)])
    right = {(0, 0): panel, (1, 0): send(panel, to_half)}
    for kept, there in ((left, lambda k: to_orb(0, k)), (right, to_x)):
        for d in range(2):
            for k in (1, 3):
                kept[d, k] = send(kept[d, 0], there(k))
        kept[0, 2] = send(kept[0, 1], there(1))
    left[1, 2] = send(left[1, 3], to_orb(0, 3))
    pieces = {n: [v] for n, v in right.items()}
    pieces[1, 2] = [send(right[1, 3], to_x(3))]
    lefts = [left[dy, k] for dy in range(2) for k in range(NZ)]
    mine = [pieces[n] for n in PANELS]
    others = [[send(v, to_core) for v in pieces[n]] for n in PANELS]
    parts = product(where, lefts, mine[:EARLY], others[:EARLY])
    parts = product(where, lefts, mine[EARLY:], others[EARLY:], parts)
    sent = {m: v for m, v in zip(MEMBERS, parts)}
    for m in ((1, 0), (1, 1), (1, 3), (1, 2), (0, 1), (0, 3), (0, 2)):
        sent[m] = send(sent[m], to_orb(*m))
    parts = [sent[m] for m in MEMBERS]
    return place(where, parts)


def solution(mesh):
    return jax.shard_map(
        exchange,
        mesh=mesh,
        in_specs=(P(None, "row", "orb"), P("orb", None)),
        out_specs=P(("row", "orb"), None),
        check_vma=False,
    )
```

```python
import functools

import jax
import jax.numpy as jnp
from jax import lax
from jax.experimental import pallas as pl
from jax.experimental.pallas import tpu as pltpu
from jax.sharding import PartitionSpec as P


AXES = ("row", "orb")
NX, NY, NZ, NC = 4, 4, 4, 2
F16_TOP = 32768.0
OTHERS = ((1, 2), (0, 2), (1, 1), (0, 1), (1, 3), (0, 3), (1, 0))
MEMBERS = ((0, 0),) + OTHERS
PANELS = ((0, 0), (1, 0), (0, 1), (0, 3), (1, 1), (1, 3), (0, 2), (1, 2))
EARLY = 6


def device_at(x, y, z, c):
    x, y, z, c = x % NX, y % NY, z % NZ, c % NC
    row = ((y // 2) * NX + x) * NC + c
    return row * 8 + (y % 2) * NZ + z


def send(value, target):
    pairs = [
        (device_at(x, y, z, c), device_at(*target(x, y, z, c)))
        for x in range(NX)
        for y in range(NY)
        for z in range(NZ)
        for c in range(NC)
    ]
    return lax.ppermute(value, AXES, pairs)


def to_orb(dy, k):
    return lambda x, y, z, c: (x, y ^ dy, z + k, c)


def to_x(k):
    return lambda x, y, z, c: (x + k, y, z, c)


def to_core(x, y, z, c):
    return x, y, z, c ^ 1


def to_panel(k):
    return lambda x, y, z, c: (x, (y & 2) | c, z + k, (y & 1) ^ c)


def to_half(x, y, z, c):
    return x, y ^ 2, z, c


def peak_of(block):
    return jnp.max(jnp.max(jnp.abs(block), axis=0, keepdims=True).astype(jnp.float32))


def pair_columns(where, k, c_ref):
    y, z = where[0], where[1]
    blocks = []
    for dy in range(2):
        start = (lax.rem(y + dy, 2) * NZ + lax.rem(z + k, NZ)) * 128
        blocks.append(c_ref[:, pl.ds(pl.multiple_of(start, 128), 128)])
    return jnp.concatenate(blocks, axis=1)


def first_kernel(k, where, l_ref, c_ref, out0, out1, bound, scale):
    terms_kernel(k, where, l_ref, c_ref, out0, out1)
    peak = peak_of(l_ref[0])
    for p in range(1, l_ref.shape[0]):
        peak = jnp.maximum(peak, peak_of(l_ref[p]))
    limit = jnp.maximum(peak * peak_of(c_ref[...]) * l_ref.shape[2], 1e-30)
    bound[...] = jnp.full(bound.shape, limit)
    scale[...] = jnp.full(bound.shape, F16_TOP / limit)


def first_terms(where, chol_vectors, orbitals, k):
    vectors, rows, contracted = chol_vectors.shape
    whole = pl.BlockSpec(memory_space=pltpu.VMEM)
    return pl.pallas_call(
        functools.partial(first_kernel, k),
        grid_spec=pltpu.PrefetchScalarGridSpec(
            num_scalar_prefetch=1, grid=(), in_specs=[whole] * 2, out_specs=[whole] * 4
        ),
        out_shape=[jax.ShapeDtypeStruct((vectors, rows, 128), jnp.float32)] * 2
        + [jax.ShapeDtypeStruct((8, 128), jnp.float32)] * 2,
        compiler_params=pltpu.CompilerParams(vmem_limit_bytes=20 << 20),
        cost_estimate=pl.CostEstimate(
            flops=2 * vectors * rows * contracted * 256, bytes_accessed=8 << 20, transcendentals=0
        ),
        name="first_terms",
    )(where, chol_vectors, orbitals)


def terms_kernel(k, where, l_ref, c_ref, out0, out1):
    columns = pair_columns(where, k, c_ref)
    for p in range(l_ref.shape[0]):
        terms = jnp.dot(l_ref[p], columns, preferred_element_type=jnp.float32)
        out0[p] = terms[:, :128]
        out1[p] = terms[:, 128:]


def more_terms(where, vecs, orbitals, k):
    vectors, rows, contracted = vecs.shape
    whole = pl.BlockSpec(memory_space=pltpu.VMEM)
    return pl.pallas_call(
        functools.partial(terms_kernel, k),
        grid_spec=pltpu.PrefetchScalarGridSpec(
            num_scalar_prefetch=1, grid=(), in_specs=[whole] * 2, out_specs=[whole] * 2
        ),
        out_shape=[jax.ShapeDtypeStruct((vectors, rows, 128), jnp.float32)] * 2,
        compiler_params=pltpu.CompilerParams(vmem_limit_bytes=20 << 20),
        cost_estimate=pl.CostEstimate(
            flops=2 * vectors * rows * contracted * 256, bytes_accessed=8 << 20, transcendentals=0
        ),
        name="more_terms",
    )(where, vecs, orbitals)


def product_kernel(parts, done, where, *refs):
    left, refs = refs[: 2 * NZ], refs[2 * NZ :]
    count = sum(parts)
    mine, others = [], []
    for pieces, flat in ((mine, refs[:count]), (others, refs[count : 2 * count])):
        for n in parts:
            pieces.append(flat[:n])
            flat = flat[n:]
    before, outs, total = refs[2 * count : -9], refs[-9:-1], refs[-1]
    y, z, c = where[0], where[1], where[4]
    vectors, width = left[0].shape[0], mine[0][0].shape[2]

    def tile(piece, k, v):
        per = NZ // len(piece)
        return piece[k // per][k % per, v]

    for ref, out in zip(before, outs):
        out[:, :done] = ref[...]
    for pair in range(0, len(parts), 2):
        value = None
        for dy in range(2):
            for k in range(NZ):
                for p in range(0, vectors, 2):
                    l = jnp.concatenate([left[dy * NZ + k][p], left[dy * NZ + k][p + 1]], axis=1)
                    blocks = []
                    for q in (pair, pair + 1):
                        row = [
                            jnp.where(c == dy, tile(mine[q], k, v), tile(others[q], k, v))
                            for v in (p, p + 1)
                        ]
                        blocks.append(jnp.concatenate(row, axis=1))
                    term = lax.dot_general(
                        l,
                        jnp.concatenate(blocks, axis=0),
                        (((1,), (1,)), ((), ())),
                        preferred_element_type=jnp.float32,
                    )
                    value = term if value is None else value + term
        total[...] = value
        for (dy, k), out in zip(MEMBERS, outs):
            start = (lax.rem(y + dy, 2) * NZ + lax.rem(z + k, NZ)) * 64
            rows = total[pl.ds(pl.multiple_of(start, 64), 64), :]
            at = done + pair * width
            out[:, at : at + 2 * width] = rows.astype(out.dtype)


def product(where, left, mine, others, before=()):
    parts = tuple(len(m) for m in mine)
    vectors, rows, depth = left[0].shape
    width = mine[0][0].shape[2]
    done = before[0].shape[1] if before else 0
    columns = done + len(parts) * width
    whole = pl.BlockSpec(memory_space=pltpu.VMEM)
    return pl.pallas_call(
        functools.partial(product_kernel, parts, done),
        grid_spec=pltpu.PrefetchScalarGridSpec(
            num_scalar_prefetch=1,
            grid=(),
            in_specs=[whole] * (2 * NZ + 2 * sum(parts) + len(before)),
            out_specs=[whole] * 8,
            scratch_shapes=[pltpu.VMEM((rows, 2 * width), jnp.float32)],
        ),
        out_shape=[
            jax.ShapeDtypeStruct((64, columns), jnp.bfloat16 if i else jnp.float32)
            for i in range(8)
        ],
        compiler_params=pltpu.CompilerParams(vmem_limit_bytes=40 << 20),
        cost_estimate=pl.CostEstimate(
            flops=4 * rows * len(parts) * width * depth * vectors * NZ,
            bytes_accessed=12 << 20,
            transcendentals=0,
        ),
        name="product",
    )(where, *left, *sum(mine, []), *sum(others, []), *before)


def place_kernel(where, *refs):
    ins, out, made, sems = refs[:8], refs[8], refs[9], refs[10]
    y, z, x, half = where[0], where[1], where[2], where[3]
    copies = []
    for n, (dh, kx) in enumerate(PANELS):
        block = lax.rem(half + dh, 2) * NX + lax.rem(x + NX - kx, NX)
        for ref, (dy, k) in zip(ins, MEMBERS):
            member = lax.rem(y + dy, 2) * NZ + lax.rem(z + NZ - k, NZ)
            at = pl.ds(pl.multiple_of(member * 128, 128), 128)
            made[n, :, at] = ref[:, n * 128 : (n + 1) * 128].astype(out.dtype)
        columns = pl.ds(pl.multiple_of(block * 1024, 1024), 1024)
        copies.append(pltpu.make_async_copy(made.at[n], out.at[:, columns], sems.at[n]))
        copies[-1].start()
    for copy in copies:
        copy.wait()


def place(where, parts):
    whole = pl.BlockSpec(memory_space=pltpu.VMEM)
    rows, columns = parts[0].shape
    return pl.pallas_call(
        place_kernel,
        grid_spec=pltpu.PrefetchScalarGridSpec(
            num_scalar_prefetch=1,
            grid=(),
            in_specs=[whole] * 8,
            out_specs=pl.BlockSpec(memory_space=pl.ANY),
            scratch_shapes=[
                pltpu.VMEM((len(PANELS), rows, 1024), jnp.float32),
                pltpu.SemaphoreType.DMA((len(PANELS),)),
            ],
        ),
        out_shape=jax.ShapeDtypeStruct((rows, columns * 8), jnp.float32),
        cost_estimate=pl.CostEstimate(flops=1 << 20, bytes_accessed=3 << 20, transcendentals=0),
        name="place",
    )(where, *parts)


def exchange(chol_vectors, orbitals):
    row, orb = lax.axis_index("row"), lax.axis_index("orb")
    z, y = orb % NZ, orb // NZ
    x, half, core = (row // NC) % NX, row // (NC * NX), row % NC
    where = jnp.stack([y, z, x, half, core]).astype(jnp.int32)

    terms = {}
    terms[0, 2], terms[1, 2], tile, scale = first_terms(where, chol_vectors, orbitals, 2)
    for k in (1, 3, 0):
        terms[0, k], terms[1, k] = more_terms(where, chol_vectors, orbitals, k)
    got = []
    for k in (2, 1, 3, 0):
        pair = (terms[0, k], terms[1, k], scale) if k else (terms[1, k], scale)
        *pair, by = lax.optimization_barrier(pair)
        pair = [(v * by[0]).astype(jnp.float16) for v in pair]
        got.append(send(pair[-1], to_orb(1, k)))
        if k:
            got.append(send(pair[0], to_orb(0, k)))
    bounds_y = (tile, send(tile, to_orb(1, 0)))
    bounds = {(1, 0): bounds_y[1][0]}
    both = jnp.concatenate(bounds_y, axis=0)
    for k in range(1, NZ):
        there = send(both, to_orb(0, k))
        bounds[0, k], bounds[1, k] = there[0], there[8]
    total = terms[0, 0]
    for i, (member, value) in enumerate(zip(OTHERS, got)):
        total = total + value.astype(jnp.float32) * (bounds[member] * (1.0 / F16_TOP))
        if i == 4:
            total = lax.optimization_barrier(total)
    half_vec = total.astype(jnp.bfloat16)

    left = {(0, 0): half_vec, (1, 0): send(half_vec, to_orb(1, 0))}
    slices = [
        lax.dynamic_slice_in_dim(half_vec, ((z + k) % NZ) * 128, 128, axis=1) for k in range(NZ)
    ]
    panel = jnp.stack([send(slices[k], to_panel(k)) for k in range(NZ)])
    right = {(0, 0): panel, (1, 0): send(panel, to_half)}
    for kept, there in ((left, lambda k: to_orb(0, k)), (right, to_x)):
        for d in range(2):
            for k in (1, 3):
                kept[d, k] = send(kept[d, 0], there(k))
        kept[0, 2] = send(kept[0, 1], there(1))
    left[1, 2] = send(left[1, 3], to_orb(0, 3))
    pieces = {n: [v] for n, v in right.items()}
    pieces[1, 2] = [send(right[1, 3], to_x(3))]
    lefts = [left[dy, k] for dy in range(2) for k in range(NZ)]
    mine = [pieces[n] for n in PANELS]
    others = [[send(v, to_core) for v in pieces[n]] for n in PANELS]
    parts = product(where, lefts, mine[:EARLY], others[:EARLY])
    parts = product(where, lefts, mine[EARLY:], others[EARLY:], parts)
    sent = {m: v for m, v in zip(MEMBERS, parts)}
    for m in ((1, 0), (1, 1), (1, 3), (1, 2), (0, 1), (0, 3), (0, 2)):
        sent[m] = send(sent[m], to_orb(*m))
    parts = [sent[m] for m in MEMBERS]
    return place(where, parts)


def solution(mesh):
    return jax.shard_map(
        exchange,
        mesh=mesh,
        in_specs=(P(None, "row", "orb"), P("orb", None)),
        out_specs=P(("row", "orb"), None),
        check_vma=False,
    )
```
